32 devices in a mesh: leaf: 8 (over z, y), front: 4 (over x, core).
Axes of the slice: x: 2, y: 2, z: 4, core: 2. Of those that a mesh axis runs over, the one named last changes fastest.
Arguments:
- right_side: float32 [8, 4, 96, 512], P('leaf', 'front'), may hold values from -6 to 6
- factor_inverse: float32 [8, 4, 128, 7680], P('leaf', 'front'), may hold values from -1 to 1, as said below
- update_panel: float32 [8, 4, 128, 1792], P('leaf', 'front'), may hold values from -0.09375 to 0.09375
- update_targets: int32 [8, 14], P('leaf'), may hold values from 0 to 31, as said below
- pivot_pairs: int32 [8, 4, 256], P('leaf', 'front'), may hold values 0 or 1
- pivot_diagonal: float32 [8, 4, 512], P('leaf', 'front'), may hold values from 0.5 to 2
- pivot_coupling: float32 [8, 4, 256], P('leaf', 'front'), may hold values from 3 to 5
Outputs:
- solution: float32 [8, 4, 96, 512], P('leaf', 'front')
The draws below stay inside these ranges and needn't reach their ends.
Inputs may be any that keep to these rules, and one draw needn't show every extreme that they name: `factor_inverse`: each front's inverse factor is lower triangular in the front's row order with ones on its diagonal. `update_targets`: each front's list names distinct blocks of its parent's pivot rows in rising order, and is repeated in the row of every leaf index of the front's group.
All inputs are finite; a program needn't handle non-finite values. No bound on the sum of `pivot_pairs` on one device may be relied on, other than what follows from the above.
Results may differ from the reference program's by a relative error of at most 0.0001.
Values sent between devices are 32-bit elements; how exact they have to be, the bound alone decides.
A program may use at most 64 MiB of HBM per device.

```python
import math
import jax
import jax.numpy as jnp
from jax import lax

PB = 128
R = 96
LEVELS = 4
BLOCK = 128
UCOLS = 1792
N_LEAF = 8
N_FRONT = 4


def draw_factor_inverse(key, part):
    leaf_ids = jnp.arange(N_LEAF, dtype=jnp.int32)[:, None, None, None]
    front_ids = jnp.arange(N_FRONT, dtype=jnp.int32)[None, :, None, None]
    row_ids = jnp.arange(PB, dtype=jnp.int32)[None, None, :, None]
    pieces = []
    for level_index in range(LEVELS):
        group_width = 2 ** level_index
        front_span = N_FRONT * PB * group_width
        column = jnp.arange(front_span, dtype=jnp.int32)[None, None, None, :]
        row_order = (front_ids * group_width + leaf_ids % group_width) * PB + row_ids
        level_key = jax.random.fold_in(key, 11 + level_index)
        shape_all = (N_LEAF, N_FRONT, PB, front_span)
        noise_part = jax.random.normal(level_key, shape_all, jnp.float32)
        noise_part = noise_part * (0.5 / math.sqrt(front_span))
        level_block = jnp.where(column < row_order, noise_part, 0.0) + jnp.where(column == row_order, 1.0, 0.0)
        pieces.append(level_block.astype(jnp.float32))
    return jnp.concatenate(pieces, axis=-1)


def draw_update_targets(key, part):
    target_lists = []
    for level_index in range(LEVELS - 1):
        group_width = 2 ** level_index
        node_count = N_LEAF // group_width
        block_count = 2 * PB * group_width // BLOCK
        parent_blocks = N_FRONT * PB * 2 * group_width // BLOCK
        scores = jax.random.randint(jax.random.fold_in(key, 31 + level_index), (node_count, parent_blocks), 0, 1 << 20)
        scores = scores * parent_blocks + jnp.arange(parent_blocks, dtype=jnp.int32)[None, :]
        node_ids = jnp.arange(node_count, dtype=jnp.int32)[:, None]
        block_ids = jnp.arange(parent_blocks, dtype=jnp.int32)[None, :]
        forced = (node_ids == 0) & (block_ids == parent_blocks - 1) | (node_ids == node_count - 1) & (block_ids == 0)
        scores = jnp.where(forced, -1, scores)
        chosen = jnp.sort(jnp.argsort(scores, axis=1)[:, :block_count].astype(jnp.int32), axis=1)
        target_lists.append(jnp.repeat(chosen, group_width, axis=0))
    return jnp.concatenate(target_lists, axis=1)


def touch_ends(entries, stream_key, least, high):
    dims = entries.shape
    index_at = [jax.random.randint(jax.random.fold_in(stream_key, axis), (), 0, dims[axis]) for axis in range(len(dims))]
    entries = entries.at[tuple(index_at)].set(least)
    longest = dims.index(max(dims))
    index_at[longest] = (index_at[longest] + 1) % dims[longest]
    return entries.at[tuple(index_at)].set(high)


def block_levels(stream_key, extent, split, least, high):
    def one(position, parts):
        heights = jax.random.uniform(jax.random.fold_in(jax.random.fold_in(stream_key, 6), position), (parts,), jnp.float32, least / len(split), high / len(split))
        return jnp.repeat(jnp.exp(heights), extent[position] // parts).reshape((-1,) + (1,) * (len(extent) - position - 1))

    factor_of = one(*split[0])
    for cut in split[1:]:
        factor_of = factor_of * one(*cut)
    return factor_of


def noise(key, dims, deviation, most, shards=(), kind=jnp.bfloat16):
    values = deviation * jax.random.normal(key, dims, jnp.float32)
    if shards:
        values = values * block_levels(key, dims, shards, -0.22, 0.18)
    return jnp.clip(values, -most, most).astype(kind)


def setup_inputs(seed: int = 0) -> dict:
    keys = jax.random.split(jax.random.key(seed), 8)
    right_side = noise(keys[0], (N_LEAF, N_FRONT, R, LEVELS * PB), 1.0, 6.0, ((0, 8), (1, 4)), jnp.float32)
    factor_inverse = draw_factor_inverse(jax.random.fold_in(keys[7], 71), 0)
    update_panel = noise(keys[2], (N_LEAF, N_FRONT, PB, UCOLS), (N_FRONT * PB * 2 ** (LEVELS - 1)) ** -0.5, 0.09375, ((0, 8), (1, 4)), jnp.float32)
    update_targets = draw_update_targets(jax.random.fold_in(keys[7], 71), 0)
    pivot_pairs = touch_ends((jax.random.randint(keys[4], (N_LEAF, N_FRONT, LEVELS * PB // 2), 0, 2) < 1).astype(jnp.int32), jax.random.fold_in(keys[4], 1), 0, 1)
    pivot_diagonal = jnp.clip(jnp.exp(math.log(2.0) - 1.3862944 * jax.random.uniform(keys[5], (N_LEAF, N_FRONT, LEVELS * PB), jnp.float32) ** block_levels(keys[5], (N_LEAF, N_FRONT, LEVELS * PB), ((0, 8), (1, 4)), -0.2, 0.2)), 0.5, 2.0)
    pivot_coupling = jnp.clip(3.0 + 2.0 * jax.random.uniform(keys[6], (N_LEAF, N_FRONT, LEVELS * PB // 2), jnp.float32) ** block_levels(keys[6], (N_LEAF, N_FRONT, LEVELS * PB // 2), ((0, 8), (1, 4)), -0.2, 0.2), 3.0, 5.0)
    return dict(right_side=right_side, factor_inverse=factor_inverse, update_panel=update_panel, update_targets=update_targets, pivot_pairs=pivot_pairs, pivot_diagonal=pivot_diagonal, pivot_coupling=pivot_coupling)


exact_mode = lax.Precision.HIGHEST


def front_of(values, level_index):
    group_width = 2 ** level_index
    node_count = N_LEAF // group_width
    side_count = values.shape[2]
    shaped = values.reshape(node_count, group_width, N_FRONT, side_count, PB)
    return shaped.transpose(0, 3, 2, 1, 4).reshape(node_count, side_count, N_FRONT * group_width * PB)


def spread_rows(front_values, level_index):
    group_width = 2 ** level_index
    node_count = N_LEAF // group_width
    side_count = front_values.shape[1]
    shaped = front_values.reshape(node_count, side_count, N_FRONT, group_width, PB)
    return shaped.transpose(0, 3, 2, 1, 4).reshape(N_LEAF, N_FRONT, side_count, PB)


def pivot_solve(solved, pivot_diag, couple, pivot_kinds):
    pair_first = solved[..., 0::2]
    second = solved[..., 1::2]
    diag_first = pivot_diag[..., 0::2][:, :, None, :]
    diag_second = pivot_diag[..., 1::2][:, :, None, :]
    coupling = couple[:, :, None, :]
    pair_flag = (pivot_kinds == 1)[:, :, None, :]
    determinant = diag_first * diag_second - coupling * coupling
    two_first = (diag_second * pair_first - coupling * second) / determinant
    two_second = (diag_first * second - coupling * pair_first) / determinant
    result_first = jnp.where(pair_flag, two_first, pair_first / diag_first)
    result_second = jnp.where(pair_flag, two_second, second / diag_second)
    return jnp.stack([result_first, result_second], axis=-1).reshape(solved.shape)


def target_table(update_targets, level_index):
    group_width = 2 ** level_index
    block_count = 2 * PB * group_width // BLOCK
    target_start = 2 * PB * (group_width - 1) // BLOCK
    parent_blocks = N_FRONT * PB * 2 * group_width // BLOCK
    target_lists = update_targets[::group_width, target_start:target_start + block_count]
    ids = jnp.arange(parent_blocks, dtype=jnp.int32)
    return (target_lists[:, :, None] == ids[None, None, :]).astype(jnp.float32)


def reference(right_side, factor_inverse, update_panel, update_targets, pivot_pairs, pivot_diagonal, pivot_coupling):
    side_count = right_side.shape[2]
    carried = jnp.zeros((N_LEAF, N_FRONT, side_count, PB), jnp.float32)
    weighted = []
    half_pb = PB // 2
    for level_index in range(LEVELS):
        group_width = 2 ** level_index
        node_count = N_LEAF // group_width
        front_span = N_FRONT * PB * group_width
        column_start = N_FRONT * PB * (group_width - 1)
        inverse_rows = factor_inverse[..., column_start:column_start + front_span]
        own_side = right_side[..., level_index * PB:(level_index + 1) * PB] - carried
        gathered = jnp.repeat(front_of(own_side, level_index), group_width, axis=0)
        solved = jnp.einsum("dqpc,drc->dqrp", inverse_rows, gathered, precision=exact_mode)
        weighted.append(pivot_solve(solved,
                                    pivot_diagonal[..., level_index * PB:(level_index + 1) * PB],
                                    pivot_coupling[..., level_index * half_pb:(level_index + 1) * half_pb],
                                    pivot_pairs[..., level_index * half_pb:(level_index + 1) * half_pb]))
        if level_index + 1 < LEVELS:
            update_len = 2 * PB * group_width
            update_start = 2 * PB * (group_width - 1)
            update_part = jnp.einsum("dqrp,dqpu->dqru", solved,
                                     update_panel[..., update_start:update_start + update_len], precision=exact_mode)
            summed = update_part.reshape(node_count, group_width, N_FRONT, side_count, update_len).sum(axis=(1, 2))
            onehot_table = target_table(update_targets, level_index)
            placed = jnp.einsum("nrkc,nkt->nrtc", summed.reshape(node_count, side_count, update_len // BLOCK, BLOCK),
                                onehot_table, precision=exact_mode)
            placed = placed.reshape(node_count // 2, 2, side_count, 2 * front_span).sum(axis=1)
            carried = spread_rows(placed, level_index + 1)
    answers = [None] * LEVELS
    for level_index in reversed(range(LEVELS)):
        group_width = 2 ** level_index
        node_count = N_LEAF // group_width
        front_span = N_FRONT * PB * group_width
        column_start = N_FRONT * PB * (group_width - 1)
        inverse_rows = factor_inverse[..., column_start:column_start + front_span]
        target = weighted[level_index]
        if level_index + 1 < LEVELS:
            update_len = 2 * PB * group_width
            update_start = 2 * PB * (group_width - 1)
            parent = jnp.repeat(front_of(answers[level_index + 1], level_index + 1), 2, axis=0)
            onehot_table = target_table(update_targets, level_index)
            chosen = jnp.einsum("nrtc,nkt->nrkc", parent.reshape(node_count, side_count, -1, BLOCK),
                                onehot_table, precision=exact_mode).reshape(node_count, side_count, update_len)
            chosen = jnp.repeat(chosen, group_width, axis=0)
            target = target - jnp.einsum("dru,dqpu->dqrp", chosen,
                                         update_panel[..., update_start:update_start + update_len], precision=exact_mode)
        partial_terms = jnp.einsum("dqrp,dqpc->dqrc", target, inverse_rows, precision=exact_mode)
        summed = partial_terms.reshape(node_count, group_width, N_FRONT, side_count, front_span).sum(axis=(1, 2))
        answers[level_index] = spread_rows(summed, level_index)
    return jnp.concatenate(answers, axis=-1)
```

```python
import functools

import jax
import jax.numpy as jnp
from jax import lax
from jax.experimental import pallas as pl
from jax.experimental.pallas import tpu as pltpu
from jax.sharding import PartitionSpec as P

LEVELS = 4
BLOCK = 128
MESH = pl.DeviceIdType.MESH
F32 = jnp.float32
BF16 = jnp.bfloat16


def flip(value, mask):
    result = value
    bit = 0
    while mask >> bit:
        if mask >> bit & 1:
            unit = 1 << bit
            result = result + (1 - 2 * lax.rem(lax.div(value, unit), 2)) * unit
        bit += 1
    return result


def split(values):
    high = values.astype(BF16)
    return high, (values - high.astype(F32)).astype(BF16)


def rows_of(values):
    high, low = split(values)
    return jnp.concatenate([high, low], 0)


def square_of(values):
    high, low = split(values)
    return jnp.concatenate(
        [jnp.concatenate([high, high], 1), jnp.concatenate([low, low], 1)], 0
    )


def along_columns(stacked, matrix):
    return lax.dot_general(
        stacked, matrix, (((1,), (1,)), ((), ())), preferred_element_type=F32
    )


def fold(product, sides, width):
    return (product[:sides, :width] + product[sides:, :width]) + (
        product[:sides, width:] + product[sides:, width:]
    )


def across(square, matrix, sides):
    product = jnp.dot(square, matrix, preferred_element_type=F32)
    return product[:sides] + product[sides:]


class Plan:
    def __init__(self, fronts, sides):
        self.fronts, self.sides = fronts, sides
        half = sides // 2
        self.gathers = {}
        self.scatters = {}
        for level in range(LEVELS):
            self.gathers["rhs", level] = (level, sides)
            self.scatters["out", level] = (level, sides)
        for level in range(LEVELS - 1):
            self.scatters["up", level] = (level, half)
            self.gathers["up", level] = (level + 1, half)
            self.scatters["down", level] = (level + 1, half)
            self.gathers["down", level] = (level, half)

    def size(self, level):
        return self.fronts << level

    def pre(self, level):
        return level >= 2


def kernel(plan, pivots, *refs):
    (
        rhs_ref,
        inverse_hbm,
        update_hbm,
        targets_ref,
        pairs_ref,
        diagonal_ref,
        coupling_ref,
        out_ref,
        inverse_raw,
        update_raw,
        inverse_split,
        update_split,
        targets_far,
        targets_smem,
        load_sem,
        targets_send,
        targets_recv,
        gather_send,
        gather_recv,
        scatter_send,
        scatter_recv,
        *buffers,
    ) = refs
    sides, fronts = plan.sides, plan.fronts
    half = sides // 2
    nx = fronts // 2
    leaf = lax.axis_index("leaf")
    front = lax.axis_index("front")
    core, column = lax.rem(front, 2), lax.div(front, 2)

    gather_keys = list(plan.gathers)
    scatter_keys = list(plan.scatters)
    gather_buffer, part, landed, first = {}, {}, {}, {}
    buffers = list(buffers)
    for key in gather_keys:
        gather_buffer[key] = buffers.pop(0)
    for key in scatter_keys:
        part[key] = buffers.pop(0)
        landed[key] = buffers.pop(0)
        if plan.pre(plan.scatters[key][0]):
            first[key] = buffers.pop(0)

    def rank(level):
        return core * (nx << level) + column * (1 << level) + lax.rem(leaf, 1 << level)

    def peer(level, mask):
        return (
            flip(leaf, mask % (1 << level)),
            flip(column, (mask >> level) % nx) * 2 + flip(core, mask // (nx << level)),
        )

    def slot_block(level, slot):
        slot_core, rest = divmod(slot, nx << level)
        slot_column, offset = divmod(rest, 1 << level)
        return ((slot_column * 2 + slot_core) << level) + offset

    def slot_of(level, block):
        index, offset = divmod(block, 1 << level)
        return (index % 2) * (nx << level) + (index // 2) * (1 << level) + offset

    sends = []

    def send(source, target, send_sem, recv_sem, device):
        pltpu.make_async_remote_copy(
            source, target, send_sem, recv_sem, device_id=device, device_id_type=MESH
        ).start()

    def wait_recv(buffer, count, send_sem, recv_sem):
        span = buffer.at[pl.ds(0, count)]
        pltpu.make_async_remote_copy(
            span, span, send_sem, recv_sem, device_id=peer(0, 1), device_id_type=MESH
        ).wait_recv()

    def wait_send(buffer, count, send_sem, recv_sem):
        span = buffer.at[pl.ds(0, count)]
        pltpu.make_async_remote_copy(
            span, span, send_sem, recv_sem, device_id=peer(0, 1), device_id_type=MESH
        ).wait_send()

    def gather_start(key):
        level, _ = plan.gathers[key]
        buffer, index = gather_buffer[key], gather_keys.index(key)
        mine = rank(level)
        sems = gather_send.at[index, 0], gather_recv.at[index, 0]
        for mask in range(1, nx << level):
            send(buffer.at[mine], buffer.at[mine], *sems, peer(level, mask))
        sends.append((buffer, (nx << level) - 1, *sems))

    def gather_forward(key):
        level, _ = plan.gathers[key]
        buffer, index = gather_buffer[key], gather_keys.index(key)
        count = nx << level
        wait_recv(buffer, count - 1, gather_send.at[index, 0], gather_recv.at[index, 0])
        span = buffer.at[pl.ds(core * count, count)]
        sems = gather_send.at[index, 1], gather_recv.at[index, 1]
        send(span, span, *sems, peer(level, count))
        sends.append((buffer, count, *sems))

    def gather_finish(key):
        level, _ = plan.gathers[key]
        index = gather_keys.index(key)
        wait_recv(
            gather_buffer[key], nx << level, gather_send.at[index, 1], gather_recv.at[index, 1]
        )

    def scatter_start(key):
        level, _ = plan.scatters[key]
        index = scatter_keys.index(key)
        count = nx << level
        if plan.pre(level):
            sems = scatter_send.at[index, 0], scatter_recv.at[index, 0]
            send(
                part[key].at[pl.ds((1 - core) * count, count)], first[key], *sems, peer(level, count)
            )
            sends.append((part[key], count, *sems))
        else:
            scatter_spread(key, 2 * count)

    def scatter_spread(key, count):
        level, _ = plan.scatters[key]
        index = scatter_keys.index(key)
        mine = rank(level)
        sems = scatter_send.at[index, 1], scatter_recv.at[index, 1]
        for mask in range(1, count):
            send(
                part[key].at[flip(mine, mask)], landed[key].at[mask - 1], *sems, peer(level, mask)
            )
        sends.append((part[key], count - 1, *sems))

    def scatter_middle(key):
        level, _ = plan.scatters[key]
        index = scatter_keys.index(key)
        count = nx << level
        if plan.pre(level):
            wait_recv(first[key], count, scatter_send.at[index, 0], scatter_recv.at[index, 0])
            span = pl.ds(core * count, count)
            part[key][span] = part[key][span] + first[key][...]
            scatter_spread(key, count)

    def scatter_finish(key):
        level, _ = plan.scatters[key]
        index = scatter_keys.index(key)
        count = (nx << level) if plan.pre(level) else fronts << level
        wait_recv(landed[key], count - 1, scatter_send.at[index, 1], scatter_recv.at[index, 1])
        total = part[key][rank(level)]
        for place in range(count - 1):
            total = total + landed[key][place]
        return total

    def column_start(level):
        return fronts * pivots * ((1 << level) - 1)

    def update_start(level):
        return 2 * pivots * ((1 << level) - 1)

    loads = []
    for level in range(LEVELS):
        cols = pl.ds(column_start(level), (fronts * pivots) << level)
        loads.append(
            pltpu.make_async_copy(
                inverse_hbm.at[0, 0, :, cols], inverse_raw.at[:, cols], load_sem.at[level]
            )
        )
    loads.append(pltpu.make_async_copy(update_hbm.at[0, 0], update_raw, load_sem.at[LEVELS]))
    loads[0].start()
    loads[LEVELS].start()
    for level in range(1, LEVELS):
        loads[level].start()

    for level in range(LEVELS):
        gather_buffer["rhs", level][rank(level)] = rhs_ref[
            0, 0, :, level * pivots : (level + 1) * pivots
        ]

    barrier = pltpu.get_barrier_semaphore()
    everyone = plan.size(LEVELS - 1)
    for mask in range(1, everyone):
        pl.semaphore_signal(
            barrier, inc=1, device_id=peer(LEVELS - 1, mask), device_id_type=MESH
        )
    pl.semaphore_wait(barrier, everyone - 1)

    gather_start(("rhs", 0))
    for level in range(LEVELS - 1):
        send(
            targets_ref,
            targets_far.at[level],
            targets_send.at[level],
            targets_recv.at[level],
            (flip(leaf, 1 << level), front),
        )
    gather_start(("rhs", 1))

    def prepare(level):
        loads[level].wait()
        for block in range(column_start(level) // BLOCK, column_start(level + 1) // BLOCK):
            high, low = split(inverse_raw[:, block * BLOCK : (block + 1) * BLOCK])
            inverse_split[block, :pivots] = high
            inverse_split[block, pivots:] = low

    def inverse_columns(start, stop):
        blocks = range(start // BLOCK, stop // BLOCK)
        return jnp.concatenate([inverse_split[block] for block in blocks], 1)

    prepare(0)
    loads[LEVELS].wait()
    high, low = split(update_raw[...])
    update_split[:pivots] = high
    update_split[pivots:] = low

    count = diagonal_ref.shape[2]
    from_pair = (
        lax.div(lax.broadcasted_iota(jnp.int32, (count // 2, count), 1), 2)
        == lax.broadcasted_iota(jnp.int32, (count // 2, count), 0)
    ).astype(F32)
    pair_rows = jnp.concatenate(
        [
            jnp.broadcast_to(coupling_ref[0], (8, count // 2)),
            jnp.broadcast_to(pairs_ref[0].astype(F32), (8, count // 2)),
        ],
        0,
    )
    repeated = jnp.dot(
        pair_rows, from_pair, precision=lax.Precision.HIGHEST, preferred_element_type=F32
    )
    couple, flags = repeated[:8], repeated[8:] > 0.5
    diagonal = jnp.broadcast_to(diagonal_ref[0], (8, count))

    def swap(values):
        width = values.shape[1]
        even = lax.rem(lax.broadcasted_iota(jnp.int32, values.shape, 1), 2) == 0
        return jnp.where(
            even, pltpu.roll(values, width - 1, 1), pltpu.roll(values, 1, 1)
        )

    other_diagonal = swap(diagonal)
    determinant = diagonal * other_diagonal - couple * couple
    straight = jnp.where(flags, other_diagonal / determinant, 1.0 / diagonal)[:1]
    crossed = jnp.where(flags, -couple / determinant, 0.0)[:1]

    def pivot_solve(solved, level):
        span = slice(level * pivots, (level + 1) * pivots)
        return solved * straight[:, span] + swap(solved) * crossed[:, span]

    for level in range(LEVELS - 1):
        pltpu.make_async_remote_copy(
            targets_ref,
            targets_far.at[level],
            targets_send.at[level],
            targets_recv.at[level],
            device_id=(flip(leaf, 1 << level), front),
            device_id_type=MESH,
        ).wait()
    lists = [targets_ref] + [targets_far.at[level] for level in range(LEVELS - 1)]
    for index, source in enumerate(lists):
        pltpu.make_async_copy(source, targets_smem.at[index], load_sem.at[LEVELS + 1]).start()
        pltpu.make_async_copy(source, targets_smem.at[index], load_sem.at[LEVELS + 1]).wait()

    def block_count(level):
        return 2 * pivots * (1 << level) // BLOCK

    def chosen_columns(level, child, index):
        place = update_start(level) // BLOCK + index
        upper = lax.rem(lax.div(leaf, 1 << level), 2)
        near, far = targets_smem[0, 0, place], targets_smem[level + 1, 0, place]
        block = near + (far - near) * (upper + child - 2 * upper * child)
        return inverse_split[column_start(level + 1) // BLOCK + block]

    def known_part(level):
        buffer = gather_buffer["rhs", level]
        product = None
        step = 2 if level else 1
        for slot in range(0, plan.size(level), step):
            start = column_start(level) + slot_block(level, slot) * pivots
            values = jnp.concatenate([buffer[slot + i] for i in range(step)], 1)
            term = along_columns(
                rows_of(values), inverse_columns(start, start + step * pivots)
            )
            product = term if product is None else product + term
        return product

    def block_at(buffer, level, child, index, parent):
        halves = []
        for place in (2 * index, 2 * index + 1):
            slot = slot_of(level, place)
            if parent:
                rank_core, rest = divmod(slot, nx << level)
                rank_column, offset = divmod(rest, 1 << level)
                slot = (
                    rank_core * (nx << (level + 1))
                    + rank_column * (1 << (level + 1))
                    + (child << level)
                    + offset
                )
            halves.append(slot)
        return halves

    weighted = []
    gather_forward(("rhs", 0))
    gather_finish(("rhs", 0))
    product = known_part(0)
    for level in range(LEVELS):
        if level:
            below = level - 1
            key = ("up", below)
            gather_finish(key)
            buffer = gather_buffer[key]
            for child in range(2):
                for index in range(0, block_count(below), 2):
                    values, matrices = [], []
                    for i in (index, index + 1):
                        low_slot, high_slot = block_at(buffer, below, child, i, True)
                        values.append(
                            jnp.concatenate([buffer[low_slot], buffer[high_slot]], 0)
                        )
                        matrices.append(chosen_columns(below, child, i))
                    product = product - along_columns(
                        rows_of(jnp.concatenate(values, 1)), jnp.concatenate(matrices, 1)
                    )
        solved = fold(product, sides, pivots)
        weighted.append(pivot_solve(solved, level))
        if level + 1 < LEVELS:
            key = ("up", level)
            start = update_start(level)
            blocks = block_count(level)
            partial = across(
                square_of(solved), update_split[:, start : start + blocks * BLOCK], sides
            )
            for index in range(blocks):
                for i, slot in enumerate(block_at(None, level, 0, index, False)):
                    part[key][slot] = partial[
                        i * half : (i + 1) * half, index * BLOCK : (index + 1) * BLOCK
                    ]
            scatter_start(key)
            prepare(level + 1)
            scatter_middle(key)
            if level == 0:
                gather_forward(("rhs", 1))
            total = scatter_finish(key)
            gather_buffer[key][rank(level + 1)] = total
            gather_start(key)
            if level + 2 < LEVELS:
                gather_start(("rhs", level + 2))
            if level:
                gather_forward(("rhs", level + 1))
            gather_finish(("rhs", level + 1))
            product = known_part(level + 1)
            gather_forward(key)

    for level in reversed(range(LEVELS)):
        target = weighted[level]
        if level + 1 < LEVELS:
            key = ("down", level)
            gather_finish(key)
            buffer = gather_buffer[key]
            product = None
            for index in range(0, block_count(level), 2):
                values = []
                for i in (index, index + 1):
                    low_slot, high_slot = block_at(buffer, level, 0, i, False)
                    values.append(jnp.concatenate([buffer[low_slot], buffer[high_slot]], 0))
                start = update_start(level) + index * BLOCK
                term = along_columns(
                    rows_of(jnp.concatenate(values, 1)),
                    update_split[:, start : start + 2 * BLOCK],
                )
                product = term if product is None else product + term
            target = target - fold(product, sides, pivots)
        square = square_of(target)
        if level:
            key = ("down", level - 1)
            for child in range(2):
                for index in range(0, block_count(level - 1), 2):
                    matrix = jnp.concatenate(
                        [chosen_columns(level - 1, child, i) for i in (index, index + 1)], 1
                    )
                    partial = across(square, matrix, sides)
                    for j in range(2):
                        places = block_at(None, level - 1, child, index + j, True)
                        for i, slot in enumerate(places):
                            part[key][slot] = partial[
                                i * half : (i + 1) * half, j * BLOCK : (j + 1) * BLOCK
                            ]
            scatter_start(key)
        out_key = ("out", level)
        step = 2 if level else 1
        for slot in range(0, plan.size(level), step):
            start = column_start(level) + slot_block(level, slot) * pivots
            partial = across(square, inverse_columns(start, start + step * pivots), sides)
            for i in range(step):
                part[out_key][slot + i] = partial[:, i * pivots : (i + 1) * pivots]
        if level:
            scatter_middle(key)
            total = scatter_finish(key)
            gather_buffer[key][rank(level - 1)] = total
            gather_start(key)
            scatter_start(out_key)
            gather_forward(key)
            scatter_middle(out_key)
        else:
            scatter_start(out_key)
            scatter_middle(out_key)
    for level in reversed(range(LEVELS)):
        out_ref[0, 0, :, level * pivots : (level + 1) * pivots] = scatter_finish(("out", level))
    for item in sends:
        wait_send(*item)


def per_device(*arguments):
    (
        right_side,
        factor_inverse,
        update_panel,
        update_targets,
        pivot_pairs,
        pivot_diagonal,
        pivot_coupling,
    ) = arguments
    pivots = factor_inverse.shape[2]
    sides = right_side.shape[2]
    fronts = lax.axis_size("front")
    plan = Plan(fronts, sides)
    nx = fronts // 2
    targets = jnp.pad(update_targets, ((0, 7), (0, BLOCK - update_targets.shape[1])))
    buffers = []
    for level, rows in plan.gathers.values():
        buffers.append(pltpu.VMEM((plan.size(level), rows, pivots), F32))
    for level, rows in plan.scatters.values():
        buffers.append(pltpu.VMEM((plan.size(level), rows, pivots), F32))
        buffers.append(pltpu.VMEM((plan.size(level), rows, pivots), F32))
        if plan.pre(level):
            buffers.append(pltpu.VMEM((nx << level, rows, pivots), F32))
    vmem = pl.BlockSpec(memory_space=pltpu.VMEM)
    hbm = pl.BlockSpec(memory_space=pl.ANY)
    dma = pltpu.SemaphoreType.DMA
    return pl.pallas_call(
        functools.partial(kernel, plan, pivots),
        out_shape=jax.ShapeDtypeStruct(right_side.shape, F32),
        in_specs=[vmem, hbm, hbm, vmem, vmem, vmem, vmem],
        out_specs=vmem,
        scratch_shapes=[
            pltpu.VMEM(factor_inverse.shape[2:], F32),
            pltpu.VMEM(update_panel.shape[2:], F32),
            pltpu.VMEM((factor_inverse.shape[3] // BLOCK, 2 * pivots, BLOCK), BF16),
            pltpu.VMEM((2 * pivots, update_panel.shape[3]), BF16),
            pltpu.VMEM((LEVELS - 1,) + targets.shape, jnp.int32),
            pltpu.SMEM((LEVELS,) + targets.shape, jnp.int32),
            dma((LEVELS + 2,)),
            dma((LEVELS - 1,)),
            dma((LEVELS - 1,)),
            dma((len(plan.gathers), 2)),
            dma((len(plan.gathers), 2)),
            dma((len(plan.scatters), 2)),
            dma((len(plan.scatters), 2)),
            *buffers,
        ],
        compiler_params=pltpu.CompilerParams(collective_id=0, has_side_effects=True),
    )(
        right_side,
        factor_inverse,
        update_panel,
        targets,
        pivot_pairs,
        pivot_diagonal,
        pivot_coupling,
    )


def solution(mesh):
    in_specs = (
        P("leaf", "front", None, None),
        P("leaf", "front", None, None),
        P("leaf", "front", None, None),
        P("leaf", None),
        P("leaf", "front", None),
        P("leaf", "front", None),
        P("leaf", "front", None),
    )
    out_specs = P("leaf", "front", None, None)
    return jax.shard_map(
        per_device, mesh=mesh, in_specs=in_specs, out_specs=out_specs, check_vma=False
    )
```

```python
import functools

import jax
import jax.numpy as jnp
from jax import lax
from jax.experimental import pallas as pl
from jax.experimental.pallas import tpu as pltpu
from jax.sharding import PartitionSpec as P

LEVELS = 4
BLOCK = 128
MESH = pl.DeviceIdType.MESH
F32 = jnp.float32
BF16 = jnp.bfloat16
PRE_FROM = 1
RELAY_FROM = 1
SHARE = 4


def flip(value, mask):
    result = value
    bit = 0
    while mask >> bit:
        if mask >> bit & 1:
            unit = 1 << bit
            result = result + (1 - 2 * lax.rem(lax.div(value, unit), 2)) * unit
        bit += 1
    return result


def split(values):
    high = values.astype(BF16)
    return high, (values - high.astype(F32)).astype(BF16)


def rows_of(values):
    high, low = split(values)
    return jnp.concatenate([high, low], 0)


def square_of(values):
    high, low = split(values)
    return jnp.concatenate(
        [jnp.concatenate([high, high], 1), jnp.concatenate([low, low], 1)], 0
    )


def along_columns(stacked, matrix):
    return lax.dot_general(
        stacked, matrix, (((1,), (1,)), ((), ())), preferred_element_type=F32
    )


def fold(product, sides, width):
    return (product[:sides, :width] + product[sides:, :width]) + (
        product[:sides, width:] + product[sides:, width:]
    )


def across(square, matrix, sides):
    product = jnp.dot(square, matrix, preferred_element_type=F32)
    return product[:sides] + product[sides:]


class Plan:
    def __init__(self, fronts, sides):
        self.fronts, self.sides = fronts, sides
        half = sides // 2
        self.gathers = {}
        self.scatters = {}
        for level in range(LEVELS):
            self.gathers["rhs", level] = (level, sides)
            self.scatters["out", level] = (level, sides)
        for level in range(LEVELS - 1):
            self.scatters["up", level] = (level, half)
            self.gathers["up", level] = (level + 1, half)
            self.scatters["down", level] = (level + 1, half)
            self.gathers["down", level] = (level, half)

    def size(self, level):
        return self.fronts << level

    def pre(self, key):
        return self.scatters[key][0] >= (1 if key[0] == "out" else PRE_FROM)

    def relay(self, key):
        return self.gathers[key][0] >= (1 if key[0] == "rhs" else RELAY_FROM)


def kernel(plan, pivots, *refs):
    (
        rhs_ref,
        inverse_hbm,
        update_hbm,
        lists_ref,
        pairs_ref,
        diagonal_ref,
        coupling_ref,
        out_ref,
        inverse_raw,
        update_raw,
        inverse_split,
        update_split,
        targets_ref,
        targets_far,
        targets_smem,
        load_sem,
        targets_send,
        targets_recv,
        gather_send,
        gather_recv,
        scatter_send,
        scatter_recv,
        *buffers,
    ) = refs
    sides, fronts = plan.sides, plan.fronts
    half = sides // 2
    nx = fronts // 2
    leaf = lax.axis_index("leaf")
    front = lax.axis_index("front")
    core, column = lax.rem(front, 2), lax.div(front, 2)

    gather_keys = list(plan.gathers)
    scatter_keys = list(plan.scatters)
    gather_buffer, part, landed, first = {}, {}, {}, {}
    buffers = list(buffers)
    for key in gather_keys:
        gather_buffer[key] = buffers.pop(0)
    for key in scatter_keys:
        part[key] = buffers.pop(0)
        landed[key] = buffers.pop(0)
        if plan.pre(key):
            first[key] = buffers.pop(0)

    def rank(level):
        return core * (nx << level) + column * (1 << level) + lax.rem(leaf, 1 << level)

    def peer(level, mask):
        return (
            flip(leaf, mask % (1 << level)),
            flip(column, (mask >> level) % nx) * 2 + flip(core, mask // (nx << level)),
        )

    def slot_block(level, slot):
        slot_core, rest = divmod(slot, nx << level)
        slot_column, offset = divmod(rest, 1 << level)
        return ((slot_column * 2 + slot_core) << level) + offset

    def slot_of(level, block):
        index, offset = divmod(block, 1 << level)
        return (index % 2) * (nx << level) + (index // 2) * (1 << level) + offset

    sends = []

    def send(source, target, send_sem, recv_sem, device):
        pltpu.make_async_remote_copy(
            source, target, send_sem, recv_sem, device_id=device, device_id_type=MESH
        ).start()

    def wait_recv(buffer, count, send_sem, recv_sem):
        span = buffer.at[pl.ds(0, count)]
        pltpu.make_async_remote_copy(
            span, span, send_sem, recv_sem, device_id=peer(0, 1), device_id_type=MESH
        ).wait_recv()

    def wait_send(buffer, count, send_sem, recv_sem):
        span = buffer.at[pl.ds(0, count)]
        pltpu.make_async_remote_copy(
            span, span, send_sem, recv_sem, device_id=peer(0, 1), device_id_type=MESH
        ).wait_send()

    bulk = []

    def issue(count):
        for _ in range(min(count, len(bulk))):
            bulk.pop(0)()

    def far_first(count):
        return sorted(range(1, count), key=lambda mask: -bin(mask).count("1"))

    def gather_start(key, later=False):
        level, _ = plan.gathers[key]
        buffer, index = gather_buffer[key], gather_keys.index(key)
        mine = rank(level)
        sems = gather_send.at[index, 0], gather_recv.at[index, 0]
        count = nx << level if plan.relay(key) else fronts << level
        for mask in far_first(count):

            def one(mask=mask):
                send(buffer.at[mine], buffer.at[mine], *sems, peer(level, mask))

            bulk.append(one) if later else one()
        sends.append((buffer, count - 1, *sems))

    def gather_forward(key):
        level, _ = plan.gathers[key]
        buffer, index = gather_buffer[key], gather_keys.index(key)
        count = nx << level
        if not plan.relay(key):
            return
        wait_recv(buffer, count - 1, gather_send.at[index, 0], gather_recv.at[index, 0])
        span = buffer.at[pl.ds(core * count, count)]
        sems = gather_send.at[index, 1], gather_recv.at[index, 1]
        send(span, span, *sems, peer(level, count))
        sends.append((buffer, count, *sems))

    def gather_finish(key):
        level, _ = plan.gathers[key]
        index = gather_keys.index(key)
        step = 1 if plan.relay(key) else 0
        count = nx << level if step else (fronts << level) - 1
        wait_recv(
            gather_buffer[key], count, gather_send.at[index, step], gather_recv.at[index, step]
        )

    def scatter_start(key):
        level, _ = plan.scatters[key]
        index = scatter_keys.index(key)
        count = nx << level
        if plan.pre(key):
            sems = scatter_send.at[index, 0], scatter_recv.at[index, 0]
            send(
                part[key].at[pl.ds((1 - core) * count, count)], first[key], *sems, peer(level, count)
            )
            sends.append((part[key], count, *sems))
        else:
            scatter_spread(key, 2 * count)

    def scatter_spread(key, count, later=False):
        level, _ = plan.scatters[key]
        index = scatter_keys.index(key)
        mine = rank(level)
        sems = scatter_send.at[index, 1], scatter_recv.at[index, 1]
        for mask in far_first(count):

            def one(mask=mask):
                send(
                    part[key].at[flip(mine, mask)],
                    landed[key].at[mask - 1],
                    *sems,
                    peer(level, mask),
                )

            bulk.append(one) if later else one()
        sends.append((part[key], count - 1, *sems))

    def scatter_middle(key, later=False):
        level, _ = plan.scatters[key]
        index = scatter_keys.index(key)
        count = nx << level
        if plan.pre(key):
            wait_recv(first[key], count, scatter_send.at[index, 0], scatter_recv.at[index, 0])
            span = pl.ds(core * count, count)
            part[key][span] = part[key][span] + first[key][...]
            scatter_spread(key, count, later)

    def scatter_finish(key):
        level, _ = plan.scatters[key]
        index = scatter_keys.index(key)
        count = (nx << level) if plan.pre(key) else fronts << level
        wait_recv(landed[key], count - 1, scatter_send.at[index, 1], scatter_recv.at[index, 1])
        total = part[key][rank(level)]
        for place in range(count - 1):
            total = total + landed[key][place]
        return total

    def column_start(level):
        return fronts * pivots * ((1 << level) - 1)

    def update_start(level):
        return 2 * pivots * ((1 << level) - 1)

    loads = []
    for level in range(LEVELS):
        cols = pl.ds(column_start(level), (fronts * pivots) << level)
        loads.append(
            pltpu.make_async_copy(
                inverse_hbm.at[0, 0, :, cols], inverse_raw.at[:, cols], load_sem.at[level]
            )
        )
    loads.append(pltpu.make_async_copy(update_hbm.at[0, 0], update_raw, load_sem.at[LEVELS]))
    loads[0].start()
    loads[LEVELS].start()
    for level in range(1, LEVELS):
        loads[level].start()

    for level in range(LEVELS):
        gather_buffer["rhs", level][rank(level)] = rhs_ref[
            0, 0, :, level * pivots : (level + 1) * pivots
        ]

    targets_ref[...] = jnp.zeros_like(targets_ref)
    targets_ref[:1, : lists_ref.shape[1]] = lists_ref[...]

    barrier = pltpu.get_barrier_semaphore()
    everyone = plan.size(LEVELS - 1)
    for mask in range(1, everyone):
        pl.semaphore_signal(
            barrier, inc=1, device_id=peer(LEVELS - 1, mask), device_id_type=MESH
        )
    pl.semaphore_wait(barrier, everyone - 1)

    gather_start(("rhs", 0))
    for level in range(LEVELS - 1):
        send(
            targets_ref,
            targets_far.at[level],
            targets_send.at[level],
            targets_recv.at[level],
            (flip(leaf, 1 << level), front),
        )
    gather_start(("rhs", 1))

    def prepare(level):
        loads[level].wait()
        for block in range(column_start(level) // BLOCK, column_start(level + 1) // BLOCK):
            high, low = split(inverse_raw[:, block * BLOCK : (block + 1) * BLOCK])
            inverse_split[block, :pivots] = high
            inverse_split[block, pivots:] = low

    def inverse_columns(start, stop):
        blocks = range(start // BLOCK, stop // BLOCK)
        return jnp.concatenate([inverse_split[block] for block in blocks], 1)

    def prepare_update(level):
        cols = slice(update_start(level), update_start(level + 1))
        high, low = split(update_raw[:, cols])
        update_split[:pivots, cols] = high
        update_split[pivots:, cols] = low

    for level in range(2, LEVELS):
        gather_start(("rhs", level), later=True)
    issue(SHARE)
    prepare(0)
    loads[LEVELS].wait()
    prepare_update(0)

    def swap(values):
        width = values.shape[1]
        even = lax.rem(lax.broadcasted_iota(jnp.int32, values.shape, 1), 2) == 0
        return jnp.where(
            even, pltpu.roll(values, width - 1, 1), pltpu.roll(values, 1, 1)
        )

    def pivot_coefficients():
        width = diagonal_ref.shape[2]
        from_pair = (
            lax.div(lax.broadcasted_iota(jnp.int32, (width // 2, width), 1), 2)
            == lax.broadcasted_iota(jnp.int32, (width // 2, width), 0)
        ).astype(F32)
        pair_rows = jnp.concatenate(
            [
                jnp.broadcast_to(coupling_ref[0], (8, width // 2)),
                jnp.broadcast_to(pairs_ref[0].astype(F32), (8, width // 2)),
            ],
            0,
        )
        repeated = jnp.dot(
            pair_rows, from_pair, precision=lax.Precision.HIGHEST, preferred_element_type=F32
        )
        couple, flags = repeated[:8], repeated[8:] > 0.5
        diagonal = jnp.broadcast_to(diagonal_ref[0], (8, width))

        other_diagonal = swap(diagonal)
        determinant = diagonal * other_diagonal - couple * couple
        straight = jnp.where(flags, other_diagonal / determinant, 1.0 / diagonal)[:1]
        crossed = jnp.where(flags, -couple / determinant, 0.0)[:1]
        return straight, crossed

    def pivot_solve(solved, level, straight, crossed):
        span = slice(level * pivots, (level + 1) * pivots)
        return solved * straight[:, span] + swap(solved) * crossed[:, span]

    def fetch_lists():
        for level in range(LEVELS - 1):
            pltpu.make_async_remote_copy(
                targets_ref,
                targets_far.at[level],
                targets_send.at[level],
                targets_recv.at[level],
                device_id=(flip(leaf, 1 << level), front),
                device_id_type=MESH,
            ).wait()
        lists = [targets_ref] + [targets_far.at[level] for level in range(LEVELS - 1)]
        copies = [
            pltpu.make_async_copy(source, targets_smem.at[index], load_sem.at[LEVELS + 1 + index])
            for index, source in enumerate(lists)
        ]
        for copy in copies:
            copy.start()
        for copy in copies:
            copy.wait()

    def block_count(level):
        return 2 * pivots * (1 << level) // BLOCK

    def chosen_columns(level, child, index):
        place = update_start(level) // BLOCK + index
        upper = lax.rem(lax.div(leaf, 1 << level), 2)
        near, far = targets_smem[0, 0, place], targets_smem[level + 1, 0, place]
        block = near + (far - near) * (upper + child - 2 * upper * child)
        return inverse_split[column_start(level + 1) // BLOCK + block]

    def known_part(level):
        buffer = gather_buffer["rhs", level]
        product = None
        step = 2 if level else 1
        for slot in range(0, plan.size(level), step):
            start = column_start(level) + slot_block(level, slot) * pivots
            values = jnp.concatenate([buffer[slot + i] for i in range(step)], 1)
            term = along_columns(
                rows_of(values), inverse_columns(start, start + step * pivots)
            )
            product = term if product is None else product + term
        return product

    def block_at(buffer, level, child, index, parent):
        halves = []
        for place in (2 * index, 2 * index + 1):
            slot = slot_of(level, place)
            if parent:
                rank_core, rest = divmod(slot, nx << level)
                rank_column, offset = divmod(rest, 1 << level)
                slot = (
                    rank_core * (nx << (level + 1))
                    + rank_column * (1 << (level + 1))
                    + (child << level)
                    + offset
                )
            halves.append(slot)
        return halves

    weighted = []
    gather_finish(("rhs", 0))
    product = known_part(0)
    for level in range(LEVELS):
        if level:
            below = level - 1
            key = ("up", below)
            gather_finish(key)
            buffer = gather_buffer[key]
            for child in range(2):
                for index in range(0, block_count(below), 2):
                    values, matrices = [], []
                    for i in (index, index + 1):
                        low_slot, high_slot = block_at(buffer, below, child, i, True)
                        values.append(
                            jnp.concatenate([buffer[low_slot], buffer[high_slot]], 0)
                        )
                        matrices.append(chosen_columns(below, child, i))
                    product = product - along_columns(
                        rows_of(jnp.concatenate(values, 1)), jnp.concatenate(matrices, 1)
                    )
        solved = fold(product, sides, pivots)
        if level + 1 < LEVELS:
            key = ("up", level)
            start = update_start(level)
            blocks = block_count(level)
            partial = across(
                square_of(solved), update_split[:, start : start + blocks * BLOCK], sides
            )
            for index in range(blocks):
                for i, slot in enumerate(block_at(None, level, 0, index, False)):
                    part[key][slot] = partial[
                        i * half : (i + 1) * half, index * BLOCK : (index + 1) * BLOCK
                    ]
            scatter_start(key)
            issue(SHARE)
            if level == 0:
                coefficients = pivot_coefficients()
            weighted.append(pivot_solve(solved, level, *coefficients))
            scatter_middle(key)
            if plan.pre(key):
                issue(SHARE)
            prepare(level + 1)
            if level + 2 < LEVELS:
                prepare_update(level + 1)
            if level == 0:
                fetch_lists()
            if level + 2 == LEVELS:
                issue(len(bulk))
            gather_forward(("rhs", level + 1))
            total = scatter_finish(key)
            gather_buffer[key][rank(level + 1)] = total
            gather_start(key)
            issue(SHARE)
            gather_finish(("rhs", level + 1))
            product = known_part(level + 1)
            gather_forward(key)
            issue(SHARE)
        else:
            weighted.append(pivot_solve(solved, level, *coefficients))

    for level in reversed(range(LEVELS)):
        target = weighted[level]
        if level + 1 < LEVELS:
            key = ("down", level)
            gather_finish(key)
            buffer = gather_buffer[key]
            product = None
            for index in range(0, block_count(level), 2):
                values = []
                for i in (index, index + 1):
                    low_slot, high_slot = block_at(buffer, level, 0, i, False)
                    values.append(jnp.concatenate([buffer[low_slot], buffer[high_slot]], 0))
                start = update_start(level) + index * BLOCK
                term = along_columns(
                    rows_of(jnp.concatenate(values, 1)),
                    update_split[:, start : start + 2 * BLOCK],
                )
                product = term if product is None else product + term
            target = target - fold(product, sides, pivots)
        square = square_of(target)
        if level:
            key = ("down", level - 1)
            for child in range(2):
                for index in range(0, block_count(level - 1), 2):
                    matrix = jnp.concatenate(
                        [chosen_columns(level - 1, child, i) for i in (index, index + 1)], 1
                    )
                    partial = across(square, matrix, sides)
                    for j in range(2):
                        places = block_at(None, level - 1, child, index + j, True)
                        for i, slot in enumerate(places):
                            part[key][slot] = partial[
                                i * half : (i + 1) * half, j * BLOCK : (j + 1) * BLOCK
                            ]
            scatter_start(key)
            scatter_middle(key)
            issue(SHARE)
        out_key = ("out", level)
        step = 2 if level else 1
        for slot in range(0, plan.size(level), step):
            start = column_start(level) + slot_block(level, slot) * pivots
            partial = across(square, inverse_columns(start, start + step * pivots), sides)
            for i in range(step):
                part[out_key][slot + i] = partial[:, i * pivots : (i + 1) * pivots]
        scatter_start(out_key)
        if level:
            total = scatter_finish(key)
            gather_buffer[key][rank(level - 1)] = total
            gather_start(key)
            scatter_middle(out_key, later=True)
            issue(SHARE)
            gather_forward(key)
            issue(SHARE)
    issue(len(bulk))
    for level in reversed(range(LEVELS)):
        out_ref[0, 0, :, level * pivots : (level + 1) * pivots] = scatter_finish(("out", level))
    for item in sends:
        wait_send(*item)


def per_device(*arguments):
    (
        right_side,
        factor_inverse,
        update_panel,
        update_targets,
        pivot_pairs,
        pivot_diagonal,
        pivot_coupling,
    ) = arguments
    pivots = factor_inverse.shape[2]
    sides = right_side.shape[2]
    fronts = lax.axis_size("front")
    plan = Plan(fronts, sides)
    nx = fronts // 2
    targets = jax.ShapeDtypeStruct((8, BLOCK), jnp.int32)
    buffers = []
    for level, rows in plan.gathers.values():
        buffers.append(pltpu.VMEM((plan.size(level), rows, pivots), F32))
    for key, (level, rows) in plan.scatters.items():
        buffers.append(pltpu.VMEM((plan.size(level), rows, pivots), F32))
        buffers.append(pltpu.VMEM((plan.size(level), rows, pivots), F32))
        if plan.pre(key):
            buffers.append(pltpu.VMEM((nx << level, rows, pivots), F32))
    vmem = pl.BlockSpec(memory_space=pltpu.VMEM)
    hbm = pl.BlockSpec(memory_space=pl.ANY)
    dma = pltpu.SemaphoreType.DMA
    return pl.pallas_call(
        functools.partial(kernel, plan, pivots),
        out_shape=jax.ShapeDtypeStruct(right_side.shape, F32),
        in_specs=[vmem, hbm, hbm, vmem, vmem, vmem, vmem],
        out_specs=vmem,
        scratch_shapes=[
            pltpu.VMEM(factor_inverse.shape[2:], F32),
            pltpu.VMEM(update_panel.shape[2:], F32),
            pltpu.VMEM((factor_inverse.shape[3] // BLOCK, 2 * pivots, BLOCK), BF16),
            pltpu.VMEM((2 * pivots, update_panel.shape[3]), BF16),
            pltpu.VMEM(targets.shape, jnp.int32),
            pltpu.VMEM((LEVELS - 1,) + targets.shape, jnp.int32),
            pltpu.SMEM((LEVELS,) + targets.shape, jnp.int32),
            dma((2 * LEVELS + 1,)),
            dma((LEVELS - 1,)),
            dma((LEVELS - 1,)),
            dma((len(plan.gathers), 2)),
            dma((len(plan.gathers), 2)),
            dma((len(plan.scatters), 2)),
            dma((len(plan.scatters), 2)),
            *buffers,
        ],
        compiler_params=pltpu.CompilerParams(collective_id=0, has_side_effects=True),
    )(
        right_side,
        factor_inverse,
        update_panel,
        update_targets,
        pivot_pairs,
        pivot_diagonal,
        pivot_coupling,
    )


def solution(mesh):
    in_specs = (
        P("leaf", "front", None, None),
        P("leaf", "front", None, None),
        P("leaf", "front", None, None),
        P("leaf", None),
        P("leaf", "front", None),
        P("leaf", "front", None),
        P("leaf", "front", None),
    )
    out_specs = P("leaf", "front", None, None)
    return jax.shard_map(
        per_device, mesh=mesh, in_specs=in_specs, out_specs=out_specs, check_vma=False
    )
```
